32 devices in a mesh: dp: 4 (over x, core), pp: 8 (over z, y).
Axes of the slice: x: 2, y: 2, z: 4, core: 2. Of those that a mesh axis runs over, the one named last changes fastest.
Arguments:
- hidden: bfloat16 [512, 4096], P(('dp', 'pp')), may hold values from -400 to 400
- norm_gain: float32 [4096], replicated, may hold values from 0.1 to 1.9
- head: bfloat16 [32768, 4096], P(('dp', 'pp')), may hold values from -32 to 32
- targets: int32 [512], P(('dp', 'pp')), may hold values from 0 to 32767
- route: int32 [32], replicated, may hold values from 0 to 3
Outputs:
- token_loss: float32 [512], P(('dp', 'pp'))
- pipe_loss: float32 [4], replicated
The draws below stay inside these ranges and needn't reach their ends.
All inputs are finite; a program needn't handle non-finite values.
Results may differ from the reference program's by a relative error of at most 0.00053.
Values may be sent and summed in bfloat16 or wider, within the bound.
A program may use at most 64 MiB of HBM per device.

```python
import math
import jax
import jax.numpy as jnp
import numpy as np
from jax import lax

D = 4096
TOK_DEV = 16
VOCAB = 32768
TOKENS = 512
N_DP = 4
N_PP = 8


def draw_hidden(key, part):
    row_scale = jnp.exp(jax.random.uniform(jax.random.fold_in(key, 11), (TOKENS, 1), jnp.float32, 0.0, 2.302585))
    col_scale = jnp.exp(jax.random.uniform(jax.random.fold_in(key, 12), (1, D), jnp.float32, 0.0, 2.302585))
    base = jnp.clip(jax.random.normal(jax.random.fold_in(key, 13), (TOKENS, D), jnp.float32), -4.0, 4.0)
    base = base * row_scale * col_scale
    return base.astype(jnp.bfloat16)


def draw_head(key, part):
    base = jnp.clip(jax.random.normal(jax.random.fold_in(key, 21), (VOCAB, D), jnp.float32), -4.0, 4.0) * (3.0 / D ** 0.5)
    return base.astype(jnp.bfloat16)


def with_ends(entries, stream_key, low, largest):
    shape = entries.shape
    spot = [jax.random.randint(jax.random.fold_in(stream_key, axis), (), 0, shape[axis]) for axis in range(len(shape))]
    entries = entries.at[tuple(spot)].set(low)
    longest = shape.index(max(shape))
    spot[longest] = (spot[longest] + 1) % shape[longest]
    return entries.at[tuple(spot)].set(largest)


def cumulative_ranks(amount, skew):
    portions = [(1 << 20) // math.isqrt(standing ** skew) + 1 for standing in range(1, amount + 1)]
    spread = 1 + sum(portions) // (1 << 30)
    return np.cumsum(np.array([max(1, weight // spread) for weight in portions]))


def ranked_ids(own_key, shape, number_of, skew):
    grid = cumulative_ranks(number_of, skew)
    ticket = jax.random.randint(jax.random.fold_in(own_key, 1), shape, 0, int(grid[number_of - 1]))
    rank = jnp.searchsorted(jnp.asarray(grid, jnp.int32), ticket, side="right")
    return jax.random.permutation(jax.random.fold_in(own_key, 2), number_of)[rank].astype(jnp.int32)


def setup_inputs(seed: int = 0) -> dict:
    seeds = jax.random.split(jax.random.key(seed), 6)
    return {
        "hidden": draw_hidden(jax.random.fold_in(seeds[5], 71), 0),
        "norm_gain": jnp.clip(1.0 + 0.18 * jax.random.normal(seeds[1], (D,), jnp.float32), 0.1, 1.9),
        "head": draw_head(jax.random.fold_in(seeds[5], 71), 0),
        "targets": with_ends(ranked_ids(seeds[3], (TOKENS,), VOCAB, 2), jax.random.fold_in(seeds[3], 3), 0, VOCAB - 1).astype(jnp.int32),
        "route": with_ends(jax.random.randint(seeds[4], (N_DP * N_PP,), 0, N_DP), jax.random.fold_in(seeds[4], 1), 0, N_DP - 1).astype(jnp.int32),
    }


def rms_normal(rows, gain):
    wide = rows.astype(jnp.float32)
    factor = lax.rsqrt(lax.optimization_barrier(jnp.mean(wide * wide, axis=1, keepdims=True)) + 1e-05)
    return (wide * factor * gain).astype(jnp.bfloat16)

def reference(hidden, norm_gain, head, targets, route):
    normed = rms_normal(hidden, norm_gain)
    block = math.gcd(TOKENS, 512)

    def one_block(pair):
        rows, marks = pair
        logits = lax.dot_general(rows, head, (((1,), (1,)), ((), ())), preferred_element_type=jnp.float32)
        peak = lax.optimization_barrier(jnp.max(logits, axis=1))
        total = peak + jnp.log(lax.optimization_barrier(jnp.sum(jnp.exp(logits - peak[:, None]), axis=1)))
        picked = jnp.take_along_axis(logits, marks[:, None].astype(jnp.int32), axis=1)[:, 0]
        return total - picked
    token_loss = lax.map(one_block, (normed.reshape(TOKENS // block, block, D), targets.reshape(TOKENS // block, block))).reshape(TOKENS)
    per_device = lax.optimization_barrier(jnp.sum(token_loss.reshape(N_DP * N_PP, TOK_DEV), axis=1))
    pick = (route[:, None] == jnp.arange(N_DP, dtype=jnp.int32)[None, :]).astype(jnp.float32)
    pipe_loss = jnp.dot(per_device, pick, precision=lax.Precision.HIGHEST) / (TOKENS // N_DP)
    return (token_loss, pipe_loss)
```

```python
import functools
import math

import jax
import jax.numpy as jnp
from jax import lax
from jax.experimental import pallas as pl
from jax.experimental.pallas import tpu as pltpu
from jax.sharding import PartitionSpec as P

CORES = 2
MESH = pl.DeviceIdType.MESH


def kernel(geom, hid, gain, tgt, route, head, out, g, hbuf, stat, loss_ref, rmap,
           recv, sends, stat_send, stat_recv, head_sem):
    nx, ny, nz, ndp, npp = geom
    devices = ndp * npp
    rows, depth = hid.shape
    half_depth = depth // 2
    width = g.shape[1]
    columns = nx * ny
    lanes = nz * CORES * rows
    vocab = hbuf.shape[0]
    vt = math.gcd(vocab, 256)

    dp, pp = lax.axis_index("dp"), lax.axis_index("pp")
    me = dp * npp + pp
    c, x = lax.rem(dp, CORES), dp // CORES
    y, z = lax.rem(pp, ny), pp // ny

    def pos_of(xx, yy, zz, cc):
        return ((xx * ny + yy) * nz + zz) * CORES + cc

    def device(xx, yy, zz, cc):
        return (xx * CORES + cc, zz * ny + yy)

    barrier = pltpu.get_barrier_semaphore()

    def greet(d, carry):
        other = lax.rem(me + d, devices)
        pl.semaphore_signal(barrier, inc=1, device_id=(other // npp, lax.rem(other, npp)),
                            device_id_type=MESH)
        return carry

    lax.fori_loop(1, devices, greet, 0)
    head_copy = pltpu.make_async_copy(head, hbuf, head_sem)
    head_copy.start()

    mine = pos_of(x, y, z, c)
    own = pl.ds(pl.multiple_of(mine * rows, rows), rows)
    wide = hid[...].astype(jnp.float32)
    factor = lax.rsqrt(jnp.mean(wide * wide, axis=1, keepdims=True) + 1e-05)
    g[own, 0:depth] = (wide * factor * gain[...]).astype(jnp.bfloat16)
    marks = jnp.broadcast_to(tgt[...], (rows, rows))
    square = (rows, rows)
    eye = lax.broadcasted_iota(jnp.int32, square, 0) == lax.broadcasted_iota(jnp.int32, square, 1)
    mark = jnp.sum(jnp.where(eye, marks, 0).astype(jnp.float32), axis=1, keepdims=True)
    high = jnp.floor(mark / 65536.0)
    rest = mark - high * 65536.0
    mid = jnp.floor(rest / 256.0)
    low = rest - mid * 256.0
    lane = lax.broadcasted_iota(jnp.int32, (rows, width - depth), 1)
    digits = jnp.where(lane == 0, low, jnp.where(lane == 1, mid, jnp.where(lane == 2, high, 0.0)))
    g[own, depth:width] = digits.astype(jnp.bfloat16)

    col = lax.broadcasted_iota(jnp.int32, (columns, lanes), 0)
    block = lax.broadcasted_iota(jnp.int32, (columns, lanes), 1) // rows
    where = col * (nz * CORES) + block
    relay = jnp.zeros((columns, lanes), jnp.int32)
    for d in range(devices):
        ddp, dpp = d // npp, d % npp
        there = pos_of(ddp // CORES, dpp % ny, dpp // ny, ddp % CORES)
        relay = jnp.where(where == there, route[d], relay)
    rmap[...] = relay

    pl.semaphore_wait(barrier, devices - 1)

    def piece(pos, half):
        part = pl.ds(0, half_depth) if half == 0 else pl.ds(half_depth, width - half_depth)
        return g.at[pl.ds(pl.multiple_of(pos * rows, rows), rows), part]

    def copy(pos, half, kind, target):
        return pltpu.make_async_remote_copy(
            src_ref=piece(pos, half),
            dst_ref=piece(pos, half),
            send_sem=sends.at[kind, half, pos // CORES],
            recv_sem=recv.at[half, pos],
            device_id=target,
            device_id_type=MESH,
        )

    partner = device(x, y, z, 1 - c)
    up, down = device(x, y, z + 1, c), device(x, y, z - 1, c)
    next_x = device(lax.rem(x + 1, nx), y, z, c)
    next_y = device(x, lax.rem(y + 1, ny), z, c)

    def arrive(half, f, s, k, sign, act):
        if half == 0:
            xx, yy = lax.rem(x - f + nx, nx), lax.rem(y - s + ny, ny)
            first, second, nf, ns = next_x, next_y, nx, ny
        else:
            xx, yy = lax.rem(x - s + nx, nx), lax.rem(y - f + ny, ny)
            first, second, nf, ns = next_y, next_x, ny, nx
        zz = z + sign * k
        there = pos_of(xx, yy, zz, c)

        def body():
            if act == "start" and (f or s or k):
                copy(there, half, 4, partner).wait_recv()

            def go(kind, target):
                cp = copy(there, half, kind, target)
                if act == "start":
                    cp.start()
                else:
                    cp.wait_send()

            if f == 0 and s == 0:
                if k == 0 or (sign < 0 and k < nz - 1):
                    pl.when(z + 1 < nz)(lambda: go(0, up))
                if k == 0 or (sign > 0 and k < nz - 1):
                    pl.when(z > 0)(lambda: go(1, down))
            if s == 0 and f < nf - 1:
                go(2, first)
            if s < ns - 1:
                go(3, second)
            go(4, partner)

        if k == 0:
            body()
        elif sign < 0:
            pl.when(z >= k)(body)
        else:
            pl.when(z + k < nz)(body)

    def column_stats(rx, ry):
        xx, yy = lax.rem(x - rx + nx, nx), lax.rem(y - ry + ny, ny)
        for zz in range(nz):
            for half in range(2):
                copy(pos_of(xx, yy, zz, 1 - c), half, 4, partner).wait_recv()
        q = xx * ny + yy
        token_rows = pl.ds(pl.multiple_of(q * lanes, lanes), lanes)
        extra = width - depth
        pick = (lax.broadcasted_iota(jnp.int32, (16, extra), 0)
                == lax.broadcasted_iota(jnp.int32, (16, extra), 1))
        digit = lax.dot_general(
            pick.astype(jnp.float32).astype(jnp.bfloat16), g[token_rows, depth:width],
            (((1,), (1,)), ((), ())), preferred_element_type=jnp.float32)
        target = digit[0:1, :] + digit[1:2, :] * 256.0 + digit[2:3, :] * 65536.0
        target = target - (me * vocab).astype(jnp.float32)

        def tile(v, carry):
            peak, mass, hit = carry
            logits = lax.dot_general(
                hbuf[pl.ds(pl.multiple_of(v * vt, vt), vt), :], g[token_rows, 0:depth],
                (((1,), (1,)), ((), ())), preferred_element_type=jnp.float32)
            ids = lax.broadcasted_iota(jnp.int32, (vt, lanes), 0) + v * vt
            top = jnp.maximum(peak, jnp.max(logits, axis=0, keepdims=True))
            mass = mass * jnp.exp(peak - top) + jnp.sum(jnp.exp(logits - top), axis=0, keepdims=True)
            hit = hit + jnp.sum(
                jnp.where(ids.astype(jnp.float32) == target, logits, 0.0), axis=0, keepdims=True)
            return top, mass, hit

        zero = jnp.zeros((1, lanes), jnp.float32)
        peak, mass, hit = lax.fori_loop(
            0, vocab // vt, tile, (jnp.full((1, lanes), -3e38, jnp.float32), zero, zero))
        stat[me, pl.ds(q, 1), :] = peak + jnp.log(mass)
        stat[me, pl.ds(columns + q, 1), :] = hit

    def events():
        found = []
        for k in range(nz):
            for f in range(max(nx, ny)):
                for s in range(max(nx, ny)):
                    found.append((k + f + s, f + s, k, f, s))
        return sorted(found)

    def legal(half, f, s):
        nf, ns = (nx, ny) if half == 0 else (ny, nx)
        return f < nf and s < ns

    def all_events(act, level=None):
        for order, _, k, f, s in events():
            if level is not None and order != level:
                continue
            for half in range(2):
                if legal(half, f, s):
                    for sign in ((-1, 1) if k else (1,)):
                        arrive(half, f, s, k, sign, act)

    last = nz - 1 + nx - 1 + ny - 1
    for level in range(last + 1):
        all_events("start", level)
        if level == nz - 1:
            head_copy.wait()
        if level >= nz - 1:
            for rx in range(nx):
                for ry in range(ny):
                    if rx + ry == level - (nz - 1):
                        column_stats(rx, ry)

    def stat_copy(source, other):
        return pltpu.make_async_remote_copy(
            src_ref=stat.at[source],
            dst_ref=stat.at[source],
            send_sem=stat_send.at[other],
            recv_sem=stat_recv.at[source],
            device_id=(other // npp, lax.rem(other, npp)),
            device_id_type=MESH,
        )

    def send_stat(d, carry):
        stat_copy(me, lax.rem(me + d, devices)).start()
        return carry

    def take_stat(d, carry):
        other = lax.rem(me + d, devices)
        stat_copy(other, other).wait_recv()
        return carry

    def sent_stat(d, carry):
        stat_copy(me, lax.rem(me + d, devices)).wait_send()
        return carry

    lax.fori_loop(1, devices, send_stat, 0)
    all_events("finish")
    lax.fori_loop(1, devices, take_stat, 0)

    every = stat[...]
    top = jnp.max(every[:, 0:columns, :], axis=0)
    mass = jnp.sum(jnp.exp(every[:, 0:columns, :] - top[None]), axis=0)
    loss = top + jnp.log(mass) - jnp.sum(every[:, columns:, :], axis=0)
    loss_ref[...] = loss
    row = jnp.broadcast_to(loss_ref[pl.ds(x * ny + y, 1), :], (8, lanes))
    shift = (z * CORES + c) * rows
    moved = pltpu.roll(row, lax.rem(lanes - shift, lanes), axis=1)
    out_lane = lax.broadcasted_iota(jnp.int32, (8, lanes), 1)
    pipes = jnp.zeros((8, lanes), jnp.float32)
    for p in range(ndp):
        total = jnp.sum(jnp.where(rmap[...] == p, loss, 0.0), keepdims=True)
        pipes = jnp.where(out_lane == p, total / (rows * devices // ndp), pipes)
    out_row = lax.broadcasted_iota(jnp.int32, (8, lanes), 0)
    out[...] = jnp.where(out_row == 0, moved, pipes)
    lax.fori_loop(1, devices, sent_stat, 0)


def shards(geom, hidden, norm_gain, head, targets, route):
    nx, ny, nz, ndp, npp = geom
    devices = ndp * npp
    rows, depth = hidden.shape
    lanes = nz * CORES * rows
    columns = nx * ny
    vmem = pl.BlockSpec(memory_space=pltpu.VMEM)
    out = pl.pallas_call(
        functools.partial(kernel, geom),
        out_shape=jax.ShapeDtypeStruct((8, lanes), jnp.float32),
        in_specs=[vmem, vmem, vmem, pl.BlockSpec(memory_space=pltpu.SMEM),
                  pl.BlockSpec(memory_space=pl.ANY)],
        out_specs=vmem,
        scratch_shapes=[
            pltpu.VMEM((rows * devices, depth + 128), jnp.bfloat16),
            pltpu.VMEM(head.shape, jnp.bfloat16),
            pltpu.VMEM((devices, 2 * columns, lanes), jnp.float32),
            pltpu.VMEM((columns, lanes), jnp.float32),
            pltpu.VMEM((columns, lanes), jnp.int32),
            pltpu.SemaphoreType.DMA((2, devices)),
            pltpu.SemaphoreType.DMA((5, 2, devices // CORES)),
            pltpu.SemaphoreType.DMA((devices,)),
            pltpu.SemaphoreType.DMA((devices,)),
            pltpu.SemaphoreType.DMA,
        ],
        compiler_params=pltpu.CompilerParams(collective_id=0, has_side_effects=True),
    )(hidden, norm_gain.reshape(1, depth), targets.reshape(1, rows), route, head)
    return out[0, :rows], out[1, :ndp]


def solution(mesh):
    ndp, npp = mesh.shape["dp"], mesh.shape["pp"]
    nx = ndp // CORES
    ny = math.gcd(nx, npp)
    geom = (nx, ny, npp // ny, ndp, npp)
    placed = (P(("dp", "pp"), None), P(), P(("dp", "pp"), None), P(("dp", "pp")), P())
    return jax.shard_map(
        functools.partial(shards, geom), mesh=mesh, in_specs=placed,
        out_specs=(P(("dp", "pp")), P()), check_vma=False
    )
```
